32 devices in a mesh: groups: 2 (over y), ctx: 4 (over z), tp: 4 (over x, core).
Axes of the slice: x: 2, y: 2, z: 4, core: 2. Of those that a mesh axis runs over, the one named last changes fastest.
Arguments:
- prompt_q: bfloat16 [1536, 8192], P(('groups', 'ctx'), 'tp'), parts along dimension 0, may hold values from -12 to 12
- prompt_k: bfloat16 [1536, 1024], P(('groups', 'ctx'), 'tp'), parts along dimension 0, may hold values from -12 to 12
- prompt_v: bfloat16 [1536, 1024], P(('groups', 'ctx'), 'tp'), parts along dimension 0, may hold values from -6 to 6
- stretch_offset: int32 [2], P('groups'), parts along dimension 0, may hold values from 0 to 32767
- step_q: bfloat16 [32, 4, 8192], P(('groups', 'ctx'), None, 'tp'), parts along dimension 0, may hold values from -12 to 12
- step_k: bfloat16 [32, 4, 1024], P(('groups', 'ctx'), None, 'tp'), parts along dimension 0, may hold values from -12 to 12
- step_v: bfloat16 [32, 4, 1024], P(('groups', 'ctx'), None, 'tp'), parts along dimension 0, may hold values from -6 to 6
- cache_len: int32 [32], P('groups'), parts along dimension 0, may hold values from 1 to 768, as said below
- slot_row: int32 [32], P('groups'), parts along dimension 0, may hold values from 0 to 15, each once
- out_weight: bfloat16 [8192, 8192], P('tp', 'ctx'), may hold values from -0.0625 to 0.0625
Outputs:
- prompt_out: bfloat16 [1536, 8192], P(('groups', 'ctx'), 'tp'), parts along dimension 0
- prompt_keys: bfloat16 [1536, 1024], P(('groups', 'ctx'), 'tp'), parts along dimension 0
- step_out: bfloat16 [32, 4, 8192], P('groups', None, ('ctx', 'tp')), parts along dimension 0
The draws below stay inside these ranges and needn't reach their ends.
There are 2 independent parts, one for each index of `groups`. The reference program is written for one: setup_inputs(seed, part) draws one part's arguments, and reference() takes and returns one part's arrays. A program takes and returns all parts, laid end to end along the dimension named above; an argument that names none is the same for every part. Nothing has to cross between parts.
Inputs may be any that keep to these rules, and one draw needn't show every extreme that they name: cache_len[r] counts the first tokens of the prompt stretch that row r's cache holds; some row holds all 768. `slot_row`: each row stands in exactly one slot.
All inputs are finite; a program needn't handle non-finite values.
Results may differ from the reference program's by a relative error of at most 0.015.
Values may be sent and summed in bfloat16 or wider, within the bound.
No kernel may reach another device: no remote copies, remote signals or barrier semaphores. Data moves between devices by JAX's collectives and lax.ppermute only.
A program may use at most 64 MiB of HBM per device.

```python
import math
import jax
import jax.numpy as jnp
from jax import lax

D = 8192
HQ = 64
KVH = 8
HD = 128
STEPS = 4
PROMPT = 768
BATCH = 16


def background(key, shape):
    return jnp.clip(jax.random.normal(key, shape, jnp.float32), -4.0, 4.0)


def draw_prompt_q(key, part):
    values = background(jax.random.fold_in(key, 21), (PROMPT, HQ * HD))
    return values.astype(jnp.bfloat16)


def draw_prompt_k(key, part):
    values = background(jax.random.fold_in(key, 22), (PROMPT, KVH * HD))
    return values.astype(jnp.bfloat16)


def draw_step_q(key, part):
    values = background(jax.random.fold_in(key, 23), (BATCH, STEPS, HQ * HD))
    return values.astype(jnp.bfloat16)


def draw_step_k(key, part):
    values = background(jax.random.fold_in(key, 24), (BATCH, STEPS, KVH * HD))
    return values.astype(jnp.bfloat16)


def draw_cache_len(key, part):
    highest = PROMPT.bit_length() - 1
    exponent = jax.random.randint(jax.random.fold_in(key, 51), (BATCH,), 0, highest + 1)
    lower = jnp.left_shift(jnp.int32(1), exponent.astype(jnp.int32))
    extra = jax.random.randint(jax.random.fold_in(key, 52), (BATCH,), 0, 1 << 30) % lower
    lengths = jnp.minimum(lower + extra, PROMPT)
    picked = jax.random.randint(jax.random.fold_in(key, 53), (), 0, BATCH)
    lengths = jnp.where(jnp.arange(BATCH) == picked, PROMPT, lengths)
    return lengths.astype(jnp.int32)


def block_scale(own_key, extent, shards, smallest, largest):
    gain = 1.0
    for axis_at, shards_of in shards:
        draws = jax.random.uniform(jax.random.fold_in(jax.random.fold_in(own_key, 6), axis_at), (shards_of,), jnp.float32, smallest / len(shards), largest / len(shards))
        gain = gain * jnp.repeat(jnp.exp(draws), extent[axis_at] // shards_of).reshape((-1,) + (1,) * (len(extent) - 1 - axis_at))
    return gain


def bell_draw(key, dims, deviation, limit, shards=(), held_as=jnp.bfloat16):
    values = deviation * jax.random.normal(key, dims, jnp.float32)
    if shards:
        values = values * block_scale(key, dims, shards, -0.22, 0.18)
    return jnp.clip(values, -limit, limit).astype(held_as)


def setup_inputs(seed: int = 0, part: int = 0) -> dict:
    seeds = jax.random.split(jax.random.key(seed), 11)
    part_keys = jax.random.split(jax.random.fold_in(seeds[10], part), 11)
    prompt_q = draw_prompt_q(jax.random.fold_in(jax.random.fold_in(seeds[10], part), 71), part)
    prompt_k = draw_prompt_k(jax.random.fold_in(jax.random.fold_in(seeds[10], part), 71), part)
    prompt_v = bell_draw(part_keys[2], (PROMPT, KVH * HD), 1.0, 6.0, ((0, 4), (1, 4)))
    stretch_offset = jax.random.randint(part_keys[3], (1,), 0, 32768).astype(jnp.int32)
    step_q = draw_step_q(jax.random.fold_in(jax.random.fold_in(seeds[10], part), 71), part)
    step_k = draw_step_k(jax.random.fold_in(jax.random.fold_in(seeds[10], part), 71), part)
    step_v = bell_draw(part_keys[6], (BATCH, STEPS, KVH * HD), 1.0, 6.0, ((0, 4), (2, 4)))
    cache_len = draw_cache_len(jax.random.fold_in(jax.random.fold_in(seeds[10], part), 71), part)
    slot_row = jax.random.permutation(part_keys[8], BATCH).astype(jnp.int32)
    out_weight = bell_draw(seeds[9], (HQ * HD, D), (HQ * HD) ** -0.5, 0.0625, ((0, 4), (1, 4)))
    return {"prompt_q": prompt_q, "prompt_k": prompt_k, "prompt_v": prompt_v, "stretch_offset": stretch_offset, "step_q": step_q, "step_k": step_k, "step_v": step_v, "cache_len": cache_len, "slot_row": slot_row, "out_weight": out_weight}


rope_base = 500000.0
floor_score = -1e30


def rotate(values, positions):
    heads = values.shape[-1] // HD
    half = HD // 2
    shaped = values.reshape(values.shape[:-1] + (heads, HD)).astype(jnp.float32)
    freqs = jnp.exp(jnp.arange(half, dtype=jnp.float32) * (-2.0 * math.log(rope_base) / HD))
    angles = positions.astype(jnp.float32)[..., None, None] * freqs
    cosine = jnp.cos(angles)
    sine = jnp.sin(angles)
    first = shaped[..., :half]
    second = shaped[..., half:]
    turned = jnp.concatenate([first * cosine - second * sine, second * cosine + first * sine], axis=-1)
    return turned.reshape(values.shape).astype(jnp.bfloat16)


def reference(prompt_q, prompt_k, prompt_v, stretch_offset, step_q, step_k, step_v, cache_len, slot_row, out_weight):
    group = HQ // KVH
    scale = HD ** -0.5
    offset = stretch_offset[0]
    prompt_pos = offset + jnp.arange(PROMPT, dtype=jnp.int32)
    prompt_query = rotate(prompt_q, prompt_pos)
    prompt_keys = rotate(prompt_k, prompt_pos)
    query_heads = prompt_query.reshape(PROMPT, KVH, group, HD).transpose(1, 2, 0, 3)
    key_heads = prompt_keys.reshape(PROMPT, KVH, HD).transpose(1, 0, 2)
    value_heads = prompt_v.reshape(PROMPT, KVH, HD).transpose(1, 0, 2)
    span = 512 if PROMPT % 512 == 0 else PROMPT
    count = PROMPT // span

    def per_head(item):
        query_group, keys_one, values_one = item
        keys_wide = keys_one.astype(jnp.float32)
        values_wide = values_one.astype(jnp.float32)

        def per_block(index):
            start = index * span
            query_block = lax.dynamic_slice_in_dim(query_group, start, span, 1).astype(jnp.float32)
            scores = jnp.einsum("gqd,kd->gqk", query_block, keys_wide) * scale
            allowed = jnp.arange(PROMPT, dtype=jnp.int32)[None, :] <= (start + jnp.arange(span, dtype=jnp.int32))[:, None]
            scores = jnp.where(allowed, scores, floor_score)
            top = scores.max(-1, keepdims=True)
            probs = jnp.where(allowed, jnp.exp(scores - top), 0.0)
            totals = probs.sum(-1)
            mixed = jnp.einsum("gqk,kd->gqd", probs.astype(jnp.bfloat16).astype(jnp.float32), values_wide)
            return (mixed / totals[..., None]).astype(jnp.bfloat16)

        blocks = lax.map(per_block, jnp.arange(count, dtype=jnp.int32))
        return blocks.transpose(1, 0, 2, 3).reshape(group, PROMPT, HD)

    heads_out = lax.map(per_head, (query_heads, key_heads, value_heads))
    prompt_out = heads_out.transpose(2, 0, 1, 3).reshape(PROMPT, HQ * HD)

    lengths = jnp.take(cache_len, slot_row).astype(jnp.int32)
    step_pos = offset + lengths[:, None] + jnp.arange(STEPS, dtype=jnp.int32)[None, :]
    step_query = rotate(step_q, step_pos)
    step_keys = rotate(step_k, step_pos)
    cache_keys = prompt_keys.reshape(PROMPT, KVH, HD).astype(jnp.float32)
    cache_values = prompt_v.reshape(PROMPT, KVH, HD).astype(jnp.float32)
    causal = jnp.arange(STEPS)[None, :] <= jnp.arange(STEPS)[:, None]

    def per_slot(item):
        query, own_keys, own_values, length = item
        query_wide = query.reshape(STEPS, KVH, group, HD).astype(jnp.float32)
        keys_near = own_keys.reshape(STEPS, KVH, HD).astype(jnp.float32)
        values_near = own_values.reshape(STEPS, KVH, HD).astype(jnp.float32)
        distant = jnp.einsum("thgd,khd->hgtk", query_wide, cache_keys) * scale
        nearby = jnp.einsum("thgd,uhd->hgtu", query_wide, keys_near) * scale
        distant_ok = jnp.arange(PROMPT, dtype=jnp.int32) < length
        distant = jnp.where(distant_ok, distant, floor_score)
        nearby = jnp.where(causal, nearby, floor_score)
        top = jnp.maximum(distant.max(-1), nearby.max(-1))[..., None]
        distant_probs = jnp.where(distant_ok, jnp.exp(distant - top), 0.0)
        nearby_probs = jnp.where(causal, jnp.exp(nearby - top), 0.0)
        totals = distant_probs.sum(-1) + nearby_probs.sum(-1)
        mixed = jnp.einsum("hgtk,khd->hgtd", distant_probs.astype(jnp.bfloat16).astype(jnp.float32), cache_values)
        mixed = mixed + jnp.einsum("hgtu,uhd->hgtd", nearby_probs.astype(jnp.bfloat16).astype(jnp.float32), values_near)
        result = (mixed / totals[..., None]).astype(jnp.bfloat16)
        return result.transpose(2, 0, 1, 3).reshape(STEPS, HQ * HD)

    attended = lax.map(per_slot, (step_query, step_keys, step_v, lengths))
    step_out = jnp.dot(attended.reshape(BATCH * STEPS, HQ * HD), out_weight, preferred_element_type=jnp.float32)
    step_out = step_out.astype(jnp.bfloat16).reshape(BATCH, STEPS, D)
    return prompt_out, prompt_keys, step_out
```

```python
import functools
import math

import jax
import jax.numpy as jnp
import numpy as np
from jax import lax
from jax.experimental import pallas as pl
from jax.experimental.pallas import tpu as pltpu
from jax.sharding import PartitionSpec as P

HQ = 64
KVH = 8
HD = 128


rope_base = 500000.0
floor_score = -1e30


def rotate(values, positions):
    heads = values.shape[-1] // HD
    half = HD // 2
    shaped = values.reshape(values.shape[:-1] + (heads, HD)).astype(jnp.float32)
    freqs = jnp.exp(jnp.arange(half, dtype=jnp.float32) * (-2.0 * math.log(rope_base) / HD))
    angles = positions.astype(jnp.float32)[..., None, None] * freqs
    cosine = jnp.cos(angles)
    sine = jnp.sin(angles)
    first = shaped[..., :half]
    second = shaped[..., half:]
    turned = jnp.concatenate(
        [first * cosine - second * sine, second * cosine + first * sine], axis=-1
    )
    return turned.reshape(values.shape).astype(jnp.bfloat16)


def fold_scores(state, scores, allowed, values, form):
    maxima, totals, weighted = state
    scores = jnp.where(allowed, scores, floor_score)
    newest = jnp.maximum(maxima, scores.max(-1))
    decay = jnp.exp(maxima - newest)
    probs = jnp.where(allowed, jnp.exp(scores - newest[..., None]), 0.0)
    totals = totals * decay + probs.sum(-1)
    weighted = weighted * decay[..., None] + jnp.einsum(
        form, probs.astype(jnp.bfloat16), values, preferred_element_type=jnp.float32
    )
    return (newest, totals, weighted)


def blank_state(leading):
    return (
        jnp.full(leading, floor_score, jnp.float32),
        jnp.zeros(leading, jnp.float32),
        jnp.zeros(leading + (HD,), jnp.float32),
    )


def decode_slots(
    step_query, step_keys, step_values, lengths, cache_keys, cache_values, kv_local, group, scale
):
    slot_rows = step_query.shape[0]
    steps = step_query.shape[1]
    query_slots = step_query.reshape(slot_rows, steps, kv_local, group, HD)
    own_keys = step_keys.reshape(slot_rows, steps, kv_local, HD)
    own_values = step_values.reshape(slot_rows, steps, kv_local, HD)
    own_scores = (
        jnp.einsum("rthgd,ruhd->rhgtu", query_slots, own_keys, preferred_element_type=jnp.float32)
        * scale
    )
    causal = jnp.arange(steps)[None, :] <= jnp.arange(steps)[:, None]
    state = fold_scores(
        blank_state((slot_rows, kv_local, group, steps)),
        own_scores,
        causal,
        own_values,
        "rhgtu,ruhd->rhgtd",
    )
    total_rows = cache_keys.shape[0]
    span = 512 if total_rows % 512 == 0 else total_rows
    keys_heads = cache_keys.reshape(total_rows, kv_local, HD)
    values_heads = cache_values.reshape(total_rows, kv_local, HD)
    needed = (jnp.max(lengths) + span - 1) // span

    def visit_block(position, current):
        key_start = (position * span).astype(jnp.int32)
        keys = lax.dynamic_slice_in_dim(keys_heads, key_start, span, 0)
        values = lax.dynamic_slice_in_dim(values_heads, key_start, span, 0)
        scores = (
            jnp.einsum("rthgd,khd->rhgtk", query_slots, keys, preferred_element_type=jnp.float32)
            * scale
        )
        allowed = (key_start + jnp.arange(span, dtype=jnp.int32))[None, :] < lengths[:, None]
        return fold_scores(
            current, scores, allowed[:, None, None, None, :], values, "rhgtk,khd->rhgtd"
        )

    state = lax.fori_loop(0, needed, visit_block, state)
    attended = (state[2] / state[1][..., None]).astype(jnp.bfloat16)
    return attended.transpose(0, 3, 1, 2, 4).reshape(slot_rows, steps, kv_local * group * HD)


def local_general(
    prompt_q,
    prompt_k,
    prompt_v,
    stretch_offset,
    step_q,
    step_k,
    step_v,
    cache_len,
    slot_row,
    out_weight,
):
    group = HQ // KVH
    scale = HD ** (-0.5)
    local_rows = prompt_q.shape[0]
    kv_local = prompt_k.shape[1] // HD
    ctx_index = lax.axis_index("ctx")
    query_start = ctx_index * local_rows
    offset = stretch_offset[0]
    prompt_pos = offset + query_start + jnp.arange(local_rows, dtype=jnp.int32)
    prompt_query = rotate(prompt_q, prompt_pos).reshape(local_rows, kv_local, group, HD)
    prompt_keys = rotate(prompt_k, prompt_pos)
    query_pos = query_start + jnp.arange(local_rows, dtype=jnp.int32)

    def attend_unit(state, keys, values, key_start):
        scores = (
            jnp.einsum("qhgd,khd->hgqk", prompt_query, keys, preferred_element_type=jnp.float32)
            * scale
        )
        key_pos = key_start + jnp.arange(keys.shape[0], dtype=jnp.int32)
        allowed = key_pos[None, :] <= query_pos[:, None]
        return fold_scores(state, scores, allowed, values, "hgqk,khd->hgqd")

    initial = blank_state((kv_local, group, local_rows))
    state = initial
    keys_all = lax.all_gather(prompt_keys, "ctx", axis=0, tiled=True).reshape(-1, kv_local, HD)
    values_all = lax.all_gather(prompt_v, "ctx", axis=0, tiled=True).reshape(-1, kv_local, HD)
    count = keys_all.shape[0]
    shards = max(1, 1024 // local_rows)
    while shards > 1 and count % (shards * local_rows) != 0:
        shards -= 1
    unit = shards * local_rows
    turns = count // unit
    keys_units = keys_all.reshape(turns, unit, kv_local, HD)
    values_units = values_all.reshape(turns, unit, kv_local, HD)

    def one_unit(carry, item):
        keys, values, position = item
        key_start = position * unit
        carry = lax.cond(
            key_start <= query_start + local_rows - 1,
            lambda current: attend_unit(current, keys, values, key_start),
            lambda current: current,
            carry,
        )
        return (carry, None)

    state, ignored = lax.scan(
        one_unit, state, (keys_units, values_units, jnp.arange(turns, dtype=jnp.int32))
    )
    cache_keys, cache_values = (
        lax.all_gather(prompt_keys, "ctx", axis=0, tiled=True),
        lax.all_gather(prompt_v, "ctx", axis=0, tiled=True),
    )
    prompt_out = (state[2] / state[1][..., None]).astype(jnp.bfloat16)
    prompt_out = prompt_out.transpose(2, 0, 1, 3).reshape(local_rows, kv_local * group * HD)
    slot_rows = step_q.shape[0]
    steps = step_q.shape[1]
    batch_rows = cache_len.shape[0]
    matches = slot_row[:, None] == jnp.arange(batch_rows, dtype=jnp.int32)[None, :]
    all_lengths = jnp.sum(jnp.where(matches, cache_len[None, :], 0), axis=1)
    my_lengths = lax.dynamic_slice_in_dim(all_lengths, ctx_index * slot_rows, slot_rows, 0)
    step_pos = offset + my_lengths[:, None] + jnp.arange(steps, dtype=jnp.int32)[None, :]
    step_query = rotate(step_q, step_pos)
    step_keys = rotate(step_k, step_pos)
    attended = decode_slots(
        step_query, step_keys, step_v, my_lengths, cache_keys, cache_values, kv_local, group, scale
    )
    columns = jnp.einsum(
        "rte,ef->rtf",
        lax.all_gather(attended, "ctx", axis=0, tiled=True),
        out_weight,
        preferred_element_type=jnp.float32,
    )
    step_out = lax.psum_scatter(columns.astype(jnp.bfloat16), "tp", scatter_dimension=2, tiled=True)
    return (prompt_out, prompt_keys, step_out)


HALF = HD // 2
LOG2E = 1.4426950408889634


def small_powers(ctx_size, tp_size):
    fits = [size in (2, 4, 8) for size in (ctx_size, tp_size)]
    return all(fits)


def frequencies():
    exponents = np.arange(HALF, dtype=np.float32) * np.float32(-2.0 * math.log(rope_base) / HD)
    freqs = np.exp(exponents).astype(np.float32)
    return jnp.asarray(np.concatenate([freqs, freqs])[None, :])


def trig_tables(positions, freqs):
    angles = positions.astype(jnp.float32) * freqs
    low = lax.broadcasted_iota(jnp.int32, angles.shape, 1) < HALF
    sine = jnp.sin(angles)
    return jnp.cos(angles), jnp.where(low, -sine, sine)


def trig_tables_folded(start, rows, freqs):
    half_rows = rows // 2
    shape = (half_rows, HD)
    low = lax.broadcasted_iota(jnp.int32, shape, 1) < HALF
    row = lax.broadcasted_iota(jnp.int32, shape, 0)
    positions = start + row + jnp.where(low, 0, half_rows)
    angles = positions.astype(jnp.float32) * freqs
    cosine = jnp.cos(angles)
    sine = jnp.sin(angles)
    cosine_back = pltpu.roll(cosine, HALF, 1)
    sine_back = pltpu.roll(sine, HALF, 1)
    cosines = jnp.concatenate(
        [jnp.where(low, cosine, cosine_back), jnp.where(low, cosine_back, cosine)], axis=0
    )
    sines = jnp.concatenate(
        [jnp.where(low, -sine, sine_back), jnp.where(low, -sine_back, sine)], axis=0
    )
    return cosines, sines


def turn(values, cosines, sines):
    wide = values.astype(jnp.float32)
    return (wide * cosines + pltpu.roll(wide, HALF, 1) * sines).astype(jnp.bfloat16)


def slot_lengths(lengths_ref, slot_row_ref, first, count):
    return [lengths_ref[slot_row_ref[first + slot]] for slot in range(count)]


def spread_rows(scalars, steps, width):
    rows = len(scalars) * steps
    row = lax.broadcasted_iota(jnp.int32, (rows, width), 0)
    spread = jnp.full((rows, width), scalars[0], jnp.int32)
    for slot in range(1, len(scalars)):
        spread = jnp.where(row >= slot * steps, scalars[slot], spread)
    return spread, row


def flat_rows(ref):
    return jnp.concatenate(
        [ref[slot].astype(jnp.float32) for slot in range(ref.shape[0])], axis=0
    )


def prepare_kernel(
    offset_ref, lengths_ref, slot_row_ref, k_ref, sq_ref, sk_ref, sv_ref, freqs_ref, keys_ref, *packs
):
    local_rows = k_ref.shape[0]
    slots, steps = sq_ref.shape[:2]
    rows = slots * steps
    ctx_index = lax.axis_index("ctx")
    offset = offset_ref[0]
    freqs = freqs_ref[...]
    cosines, sines = trig_tables_folded(offset + ctx_index * local_rows, local_rows, freqs)
    own = slot_lengths(lengths_ref, slot_row_ref, ctx_index * slots, slots)
    spread, row = spread_rows(own, steps, HD)
    step_cos, step_sin = trig_tables(offset + spread + row % steps, freqs)
    queries = flat_rows(sq_ref)
    step_keys = flat_rows(sk_ref)
    step_values = flat_rows(sv_ref)
    kv_local = len(packs)
    group = sq_ref.shape[2] // HD // kv_local
    for g in range(kv_local):
        span = slice(g * HD, (g + 1) * HD)
        turned = turn(k_ref[:, span], cosines, sines)
        keys_ref[:, span] = turned
        packs[g][:local_rows] = turned
        at = local_rows
        for h in range(group):
            lane = (g * group + h) * HD
            packs[g][at : at + rows] = turn(queries[:, lane : lane + HD], step_cos, step_sin)
            at += rows
        packs[g][at : at + rows] = turn(step_keys[:, span], step_cos, step_sin)
        packs[g][at + rows : at + 2 * rows] = step_values[:, span].astype(jnp.bfloat16)


def rotate_queries_kernel(offset_ref, q_ref, freqs_ref, out_ref):
    local_rows = q_ref.shape[0]
    start = offset_ref[0] + lax.axis_index("ctx") * local_rows
    cosines, sines = trig_tables_folded(start, local_rows, freqs_ref[...])
    for h in range(q_ref.shape[1] // HD):
        span = slice(h * HD, (h + 1) * HD)
        out_ref[:, span] = turn(q_ref[:, span], cosines, sines)


def column_positions(shape, masks, local_rows, ctx_index):
    column = lax.broadcasted_iota(jnp.int32, shape, 1)
    position = column
    for at, mask in enumerate(masks):
        source = lax.bitwise_xor(ctx_index, jnp.int32(mask))
        inside = column >= at * local_rows
        position = jnp.where(inside, column + (source - at) * local_rows, position)
    return column, position


def softmax_apply(scores, values, scale):
    top = jnp.max(scores, axis=1, keepdims=True)
    probs = jnp.exp2((scores - top) * (scale * LOG2E))
    total = jnp.sum(probs, axis=1, keepdims=True)
    mixed = jnp.dot(probs.astype(jnp.bfloat16), values, preferred_element_type=jnp.float32)
    return mixed / total


def score(queries, keys):
    return lax.dot_general(
        queries, keys, (((1,), (1,)), ((), ())), preferred_element_type=jnp.float32
    )


def prompt_kernel(*refs, masks, head, group, scale, aliased):
    count = len(masks)
    q_ref = refs[0]
    packs = refs[1 : 1 + count]
    values = refs[1 + count : 1 + 2 * count]
    out_ref = refs[1 + 2 * count + (1 if aliased else 0)]
    local_rows = q_ref.shape[0]
    ctx_index = lax.axis_index("ctx")
    span = slice(head * HD, (head + 1) * HD)
    keys_all = jnp.concatenate([pack[:local_rows] for pack in packs], axis=0)
    values_all = jnp.concatenate([value[:, span] for value in values], axis=0)
    shape = (local_rows, count * local_rows)
    _, position = column_positions(shape, masks, local_rows, ctx_index)
    mine = ctx_index * local_rows + lax.broadcasted_iota(jnp.int32, shape, 0)
    bias = jnp.where(position <= mine, 0.0, floor_score)
    for h in range(group):
        lanes = slice(h * HD, (h + 1) * HD)
        scores = score(q_ref[:, lanes], keys_all) + bias
        out_ref[:, lanes] = softmax_apply(scores, values_all, scale).astype(jnp.bfloat16)


def decode_kernel(*refs, masks, head, group, slots, steps, scale, blocks, first, last):
    count = len(masks)
    lengths_ref, slot_row_ref = refs[:2]
    packs = refs[2 : 2 + count]
    values = refs[2 + count : 2 + 2 * count]
    weight_ref = refs[2 + 2 * count]
    at = 3 + 2 * count
    carried_ref = None
    if not first:
        carried_ref = refs[at]
        at += 1
    scratch = refs[-3:]
    outs = refs[at:-3]
    weights, attended, sems = scratch
    width = weights.shape[2]
    depth = group * HD
    order = range(blocks)
    tp_index = lax.axis_index("tp")
    copies = []
    for block in order:
        copy = pltpu.make_async_copy(
            weight_ref.at[pl.ds(head * depth, depth), pl.ds(block * width, width)],
            weights.at[block],
            sems.at[block],
        )
        copy.start()
        copies.append(copy)
    rows = slots * steps
    local_rows = values[0].shape[0]
    ctx_index = lax.axis_index("ctx")
    span = slice(head * HD, (head + 1) * HD)
    base = local_rows
    keys_at = base + group * rows
    vals_at = keys_at + rows
    keys_all = jnp.concatenate(
        [pack[:local_rows] for pack in packs] + [pack[keys_at:vals_at] for pack in packs], axis=0
    )
    values_all = jnp.concatenate(
        [value[:, span] for value in values] + [pack[vals_at : vals_at + rows] for pack in packs],
        axis=0,
    )
    cached = count * local_rows
    shape = (rows, cached + count * rows)
    column, position = column_positions(shape, masks, local_rows, ctx_index)
    for j, mask in enumerate(masks):
        source = lax.bitwise_xor(ctx_index, jnp.int32(mask))
        spread, row = spread_rows(
            slot_lengths(lengths_ref, slot_row_ref, source * slots, slots), steps, shape[1]
        )
        step_column = column - (cached + j * rows)
        near = (step_column >= row - row % steps) & (step_column <= row)
        allowed = ((column < cached) & (position < spread)) | near
        bias = jnp.where(allowed, 0.0, floor_score)
        scores = score(packs[j][base:keys_at], keys_all)
        scores = (scores.reshape(group, rows, shape[1]) + bias[None]).reshape(
            group * rows, shape[1]
        )
        mixed = softmax_apply(scores, values_all, scale).astype(jnp.bfloat16)
        target = pl.ds(pl.multiple_of(source * rows, rows), rows)
        for h in range(group):
            attended[target, h * HD : (h + 1) * HD] = mixed[h * rows : (h + 1) * rows]
    for copy in copies:
        copy.wait()
    everything = attended[...]
    for relative in list(range(1, blocks, 2)) + list(range(0, blocks, 2)):
        block = lax.bitwise_xor(tp_index, jnp.int32(relative))
        product = jnp.dot(everything, weights[block], preferred_element_type=jnp.float32)
        if not first:
            product = product + carried_ref[relative]
        if not last:
            outs[0][relative] = product
        elif relative % 2:
            for slot in range(count * slots):
                outs[0][relative // 2, slot] = product[slot * steps : (slot + 1) * steps].astype(
                    jnp.bfloat16
                )
        else:
            for slot in range(count * slots):
                outs[1 + relative // 2][slot] = product[slot * steps : (slot + 1) * steps]


def swap(value, axis, mask):
    size = lax.axis_size(axis)
    return lax.ppermute(value, axis, [(i, i ^ mask) for i in range(size)])


def gather_swaps(value, axis):
    items = [value]
    bit = lax.axis_size(axis) // 2
    while bit:
        items = items + [swap(item, axis, bit) for item in items]
        bit //= 2
    return items


def gather_masks(axis):
    masks = [0]
    bit = lax.axis_size(axis) // 2
    while bit:
        masks = masks + [mask | bit for mask in masks]
        bit //= 2
    return tuple(masks)


def local_fast(
    prompt_q,
    prompt_k,
    prompt_v,
    stretch_offset,
    step_q,
    step_k,
    step_v,
    cache_len,
    slot_row,
    out_weight,
):
    scale = HD ** (-0.5)
    bf16 = jnp.bfloat16
    f32 = jnp.float32
    local_rows = prompt_q.shape[0]
    kv_local = prompt_k.shape[1] // HD
    group = HQ // KVH
    slots, steps = step_q.shape[:2]
    rows = slots * steps
    masks = gather_masks("ctx")
    count = len(masks)
    blocks = lax.axis_size("tp")
    width = out_weight.shape[1] // blocks
    smem = pl.BlockSpec(memory_space=pltpu.SMEM)
    vmem = pl.BlockSpec(memory_space=pltpu.VMEM)
    hbm = pl.BlockSpec(memory_space=pl.ANY)
    freqs = frequencies()
    pack_rows = local_rows + (group + 2) * rows

    all_values = gather_swaps(prompt_v, "ctx")
    prompt_keys, *own_packs = pl.pallas_call(
        prepare_kernel,
        out_shape=[jax.ShapeDtypeStruct(prompt_k.shape, bf16)]
        + [jax.ShapeDtypeStruct((pack_rows, HD), bf16)] * kv_local,
        in_specs=[smem] * 3 + [vmem] * 5,
        out_specs=[vmem] * (1 + kv_local),
        name="prepare",
    )(stretch_offset, cache_len, slot_row, prompt_k, step_q, step_k, step_v, freqs)
    all_packs = [gather_swaps(pack, "ctx") for pack in own_packs]
    queries = pl.pallas_call(
        rotate_queries_kernel,
        out_shape=jax.ShapeDtypeStruct(prompt_q.shape, bf16),
        in_specs=[smem, vmem, vmem],
        out_specs=vmem,
        name="rotate_queries",
    )(stretch_offset, prompt_q, freqs)

    carried = None
    prompt_out = None
    for g in range(kv_local):
        first = g == 0
        last = g == kv_local - 1
        if last:
            shape = (count * slots, steps, width)
            out_shape = [jax.ShapeDtypeStruct((blocks // 2,) + shape, bf16)]
            out_shape += [jax.ShapeDtypeStruct(shape, f32)] * (blocks // 2)
        else:
            out_shape = [jax.ShapeDtypeStruct((blocks, count * rows, width), f32)]
        carried = pl.pallas_call(
            functools.partial(
                decode_kernel,
                masks=masks,
                head=g,
                group=group,
                slots=slots,
                steps=steps,
                scale=scale,
                blocks=blocks,
                first=first,
                last=last,
            ),
            out_shape=out_shape,
            in_specs=[smem] * 2 + [vmem] * (2 * count) + [hbm] + ([] if first else [vmem]),
            out_specs=[vmem] * len(out_shape),
            scratch_shapes=[
                pltpu.VMEM((blocks, group * HD, width), bf16),
                pltpu.VMEM((count * rows, group * HD), bf16),
                pltpu.SemaphoreType.DMA((blocks,)),
            ],
            name=f"decode_{g}",
        )(
            cache_len,
            slot_row,
            *all_packs[g],
            *all_values,
            out_weight,
            *([] if first else [carried[0]]),
        )
        half = pl.BlockSpec((local_rows, group * HD), lambda i, g=g: (0, g))
        whole = lambda shape: pl.BlockSpec(shape, lambda i: (0, 0))
        prompt_out = pl.pallas_call(
            functools.partial(
                prompt_kernel, masks=masks, head=g, group=group, scale=scale, aliased=not first
            ),
            grid=(1,),
            out_shape=jax.ShapeDtypeStruct(prompt_q.shape, bf16),
            in_specs=[half]
            + [whole((pack_rows, HD))] * count
            + [whole(prompt_v.shape)] * count
            + ([] if first else [hbm]),
            out_specs=half,
            input_output_aliases={} if first else {1 + 2 * count: 0},
            name=f"prompt_{g}",
        )(queries, *all_packs[g], *all_values, *([] if first else [prompt_out]))

    sent, *kept = carried
    bit = 1
    while bit < blocks:
        received = swap(sent, "tp", bit)
        kept = [value + received[at].astype(f32) for at, value in enumerate(kept)]
        bit *= 2
        if bit < blocks:
            sent = jnp.stack([value.astype(bf16) for value in kept[1::2]])
            kept = kept[0::2]
    step_out = kept[0].astype(bf16)
    return (prompt_out, prompt_keys, step_out)


def solution(mesh):
    body = local_fast if small_powers(mesh.shape["ctx"], mesh.shape["tp"]) else local_general
    in_specs = (
        P(("groups", "ctx"), "tp"),
        P(("groups", "ctx"), "tp"),
        P(("groups", "ctx"), "tp"),
        P("groups"),
        P(("groups", "ctx"), None, "tp"),
        P(("groups", "ctx"), None, "tp"),
        P(("groups", "ctx"), None, "tp"),
        P("groups"),
        P("groups"),
        P("tp", "ctx"),
    )
    out_specs = (
        P(("groups", "ctx"), "tp"),
        P(("groups", "ctx"), "tp"),
        P("groups", None, ("ctx", "tp")),
    )
    return jax.shard_map(body, mesh=mesh, in_specs=in_specs, out_specs=out_specs, check_vma=False)
```
